32 devices in a mesh: rep: 1, r: 8 (over y, z), s: 4 (over x, core).
Axes of the slice: x: 2, y: 2, z: 4, core: 2. Of those that a mesh axis runs over, the one named last changes fastest.
Arguments:
- x: bfloat16 [32, 4096, 896], P(('rep', 'r', 's'))
- dy: bfloat16 [32, 4096, 896], P(('rep', 'r', 's'))
- w_gate: bfloat16 [2, 896, 2304], P(None, 's')
- w_up: bfloat16 [2, 896, 2304], P(None, 's')
- w_down: bfloat16 [2, 2304, 896], P(None, 's')
- m_w_gate: float32 [2, 896, 2304], P(None, 's')
- m_w_up: float32 [2, 896, 2304], P(None, 's')
- m_w_down: float32 [2, 2304, 896], P(None, 's')
- v_w_gate: float32 [2, 896, 2304], P(None, 's')
- v_w_up: float32 [2, 896, 2304], P(None, 's')
- v_w_down: float32 [2, 2304, 896], P(None, 's')
Outputs:
- output 1: bfloat16 [2, 896, 2304], P('rep', 's')
- output 2: bfloat16 [2, 896, 2304], P('rep', 's')
- output 3: bfloat16 [2, 2304, 896], P('rep', 's')
- output 4: float32 [2, 896, 2304], P('rep', 's')
- output 5: float32 [2, 896, 2304], P('rep', 's')
- output 6: float32 [2, 2304, 896], P('rep', 's')
- output 7: float32 [2, 896, 2304], P('rep', 's')
- output 8: float32 [2, 896, 2304], P('rep', 's')
- output 9: float32 [2, 2304, 896], P('rep', 's')
All inputs are finite; a program needn't handle non-finite values.
Results may differ from the reference program's by a relative error of at most 0.022.
Values are sent between devices in bfloat16 or wider.
A program may use at most 2 GiB of HBM per device.

```python
import jax
import jax.numpy as jnp
from jax import lax

SEQUENCES = 32
TOKENS = 4096
D = 896
FF = 2304
LAYERS = 2
NAMES = ("w_gate", "w_up", "w_down")
SHAPES = {"w_gate": (LAYERS, D, FF), "w_up": (LAYERS, D, FF), "w_down": (LAYERS, FF, D)}


def bump(key, n, height):
    away = (jnp.arange(n, dtype=jnp.int32) - jax.random.randint(key, (), 0, n, jnp.int32)) % n
    return jnp.where(away < n // 8, height, 1.0)


def together(key, own, strength):
    shared = jax.random.normal(key, own.shape[1:], jnp.float32)
    return (own + strength * shared) * lax.rsqrt(1 + strength * strength)


def setup_inputs(seed: int = 0, part: int = 0) -> dict:
    kx, kdy, ka, kb, kz, kf, kh, kl, *keys = jax.random.split(jax.random.key(seed), 8 + 3 * len(NAMES))
    kx, kdy, ka, kb = (jax.random.fold_in(k, part) for k in (kx, kdy, ka, kb))
    kw, km, kv = (keys[i::3] for i in range(3))
    shape = (SEQUENCES, TOKENS, D)
    much_x, much_dy = jax.random.uniform(kz, (2,), jnp.float32, 0.0, 1.0)
    loud = 2.0 ** jax.random.uniform(jax.random.fold_in(kz, 1), (), jnp.float32, -1.0, 2.0)
    layers = 2.0 ** jax.random.uniform(kl, (LAYERS, 1, 1), jnp.float32, -1.0, 1.0)
    x = together(ka, jax.random.normal(kx, shape, jnp.float32), much_x) * bump(kf, D, 4.0)
    dy = together(kb, jax.random.normal(kdy, shape, jnp.float32), much_dy)
    drawn = {"x": x.astype(jnp.bfloat16), "dy": (loud * dy * (SEQUENCES * TOKENS) ** -0.5).astype(jnp.bfloat16)}
    for key, name in zip(kw, NAMES, strict=True):
        w = jax.random.normal(key, SHAPES[name], jnp.float32) * SHAPES[name][1] ** -0.5
        drawn[name] = (w * {"w_gate": 1.0, "w_up": bump(kh, FF, 4.0), "w_down": layers}[name]).astype(jnp.bfloat16)
    for key, name in zip(km, NAMES, strict=True):
        drawn[f"m_{name}"] = 0.1 * jax.random.normal(key, SHAPES[name], jnp.float32)
    for key, name in zip(kv, NAMES, strict=True):
        drawn[f"v_{name}"] = jax.random.uniform(key, SHAPES[name], jnp.float32, 0.005, 0.015)
    return drawn


def matmul(a, w):
    return jnp.dot(a, w, preferred_element_type=jnp.float32).astype(jnp.bfloat16)


def normed(h):
    wide = h.astype(jnp.float32)
    scale = lax.rsqrt(jnp.mean(wide**2, -1, keepdims=True) + 1e-6)
    return (wide * scale).astype(jnp.bfloat16)


def layer(h, w):
    a = normed(h)
    gate = jnp.dot(a, w["w_gate"], preferred_element_type=jnp.float32)
    up = jnp.dot(a, w["w_up"], preferred_element_type=jnp.float32)
    return h + matmul((jax.nn.silu(gate) * up).astype(jnp.bfloat16), w["w_down"])


def adamw(w, m, v, g):
    m = 0.9 * m + 0.1 * g
    v = 0.95 * v + 0.05 * g * g
    step = m * lax.rsqrt(v + 1e-8) + 0.1 * w
    return (w - 0.02 * step).astype(jnp.bfloat16), m, v


def clipped(gradients, sum_of_squares, count):
    factor = jnp.minimum(1.0, 0.5 * lax.rsqrt(sum_of_squares / count + 1e-30))
    return [g * factor for g in gradients]


def stack(weights, h):
    return lax.scan(lambda h, w: (layer(h, w), None), h, weights)[0]


def reference(x, dy, w_gate, w_up, w_down, m_w_gate, m_w_up, m_w_down, v_w_gate, v_w_up, v_w_down):
    weights = dict(zip(NAMES, (w_gate, w_up, w_down), strict=True))

    def take(so_far, sequence):
        h, by_y = sequence
        _, back = jax.vjp(lambda w: stack(w, h), weights)
        return jax.tree.map(lambda total, term: total + term.astype(jnp.float32), so_far, back(by_y)[0]), None

    none_yet = {name: jnp.zeros(w.shape, jnp.float32) for name, w in weights.items()}
    by_weights, _ = lax.scan(take, none_yet, (x, dy))
    gradients = [by_weights[name].astype(jnp.bfloat16).astype(jnp.float32) for name in NAMES]
    gradients = clipped(gradients, sum(jnp.sum(g * g) for g in gradients), sum(g.size for g in gradients))
    new = [
        adamw(w.astype(jnp.float32), m, v, g)
        for w, m, v, g in zip((w_gate, w_up, w_down), (m_w_gate, m_w_up, m_w_down), (v_w_gate, v_w_up, v_w_down), gradients, strict=True)
    ]
    return tuple(one[which] for which in range(3) for one in new)
```

```python
import functools

import jax
import jax.numpy as jnp
from jax import lax
from jax.experimental import pallas as pl
from jax.experimental.pallas import tpu as pltpu
from jax.sharding import PartitionSpec as P

bf16, f32 = jnp.bfloat16, jnp.float32
MESH = pl.DeviceIdType.MESH
MIB = 2**20


def nn(a, b):
    return jnp.dot(a, b, preferred_element_type=f32)


def nt(a, b):
    return lax.dot_general(a, b, (((1,), (1,)), ((), ())), preferred_element_type=f32)


def tn(a, b):
    return lax.dot_general(a, b, (((0,), (0,)), ((), ())), preferred_element_type=f32)


def normed(h):
    wide = h.astype(f32)
    scale = lax.rsqrt(jnp.mean(wide * wide, -1, keepdims=True) + 1e-6)
    return wide, scale, (wide * scale).astype(bf16)


def backward(dact, gate, up):
    sig = lax.logistic(gate)
    silu = gate * sig
    return silu, dact * up * (sig + silu * (1.0 - sig)), dact * silu


def spread(act_ref, k, act):
    for e in range(4):
        block, third = divmod(4 * k + e, 3)
        act_ref[:, 768 * third + 192 * block : 768 * third + 192 * (block + 1)] = act[:, 192 * e : 192 * (e + 1)]


def first_kernel(
    x_ref, bg, bu, bd, a_ref, act_ref, g_ref, u_ref, h_ref, wg1, wu1, wd1, wd0, wg, wu, wd, held, send, recv, local
):
    i = pl.program_id(0)
    last = pl.num_programs(0) - 1
    r, s = lax.axis_index("r"), lax.axis_index("s")
    y, c = r // 4, s % 2
    core, across, other = s + 1 - 2 * c, lax.rem(s + 2, 4), lax.rem(r + 4, 8)
    blocks = [bg.at[0], bu.at[0], bd.at[0], bg.at[1], bu.at[1], bd.at[1]]
    wholes = [wg, wu, wd, wg1, wu1, wd1]

    def copy(m, kind):
        rows = blocks[m].shape[0]
        half = rows // 2
        whole = wholes[m]

        def remote(src, dst, rr, ss):
            return pltpu.make_async_remote_copy(
                src_ref=src,
                dst_ref=dst,
                send_sem=send.at[m, kind],
                recv_sem=recv.at[m, kind],
                device_id=(0, rr, ss),
                device_id_type=MESH,
            )

        if kind == 0:
            return remote(blocks[m], whole.at[pl.ds(s * rows, rows)], r, core)
        if kind == 1:
            return remote(blocks[m].at[pl.ds(y * half, half)], whole.at[pl.ds(s * rows + y * half, half)], r, across)
        which = y if kind in (2, 3) else 1 - y
        part = whole.at[pl.ds(across * rows + which * half, half)]
        return remote(part, part, other if kind == 2 else r, s if kind == 2 else core)

    def own(m):
        rows = blocks[m].shape[0]
        return pltpu.make_async_copy(blocks[m], wholes[m].at[pl.ds(s * rows, rows)], local.at[m])

    def crossed(m):
        copy(m, 1).wait_recv()
        copy(m, 2).start()
        copy(m, 3).start()

    def turned(m):
        copy(m, 2).wait_recv()
        copy(m, 4).start()

    def arrived(m):
        own(m).wait()
        for kind in (0, 3, 4):
            copy(m, kind).wait_recv()

    @pl.when(i == 0)
    def _():
        barrier = pltpu.get_barrier_semaphore()
        for rr, ss in ((r, core), (r, across), (other, s)):
            pl.semaphore_signal(barrier, inc=1, device_id=(0, rr, ss), device_id_type=MESH)
        pl.semaphore_wait(barrier, 3)
        for m in range(6):
            copy(m, 1).start()
            own(m).start()
            if m < 3:
                copy(m, 0).start()

    x = x_ref[...]
    _, _, a = normed(x)
    a_ref[...] = a

    @pl.when(i == 0)
    def _():
        crossed(0)
        crossed(1)
        turned(0)
        turned(1)
        arrived(0)
        arrived(1)

    for k in range(3):
        cols = slice(k * 768, (k + 1) * 768)
        gate, up = nn(a, wg[:, cols]), nn(a, wu[:, cols])
        g_ref[:, cols] = gate
        u_ref[:, cols] = up
        act = (gate * lax.logistic(gate) * up).astype(bf16)
        held[:, cols] = act
        spread(act_ref, k, act)

    @pl.when(i == 0)
    def _():
        crossed(2)
        turned(2)
        arrived(2)
        pltpu.make_async_copy(wd, wd0, local.at[6]).start()
        crossed(3)
        copy(3, 0).start()

    h_ref[...] = x + nn(held[...], wd[...]).astype(bf16)

    @pl.when(i == 1)
    def _():
        crossed(4)
        copy(4, 0).start()
        turned(3)

    @pl.when(i == 2)
    def _():
        crossed(5)
        copy(5, 0).start()
        turned(4)

    @pl.when(i == 4)
    def _():
        turned(5)

    @pl.when(i == last)
    def _():
        for m in (3, 4, 5):
            arrived(m)
        pltpu.make_async_copy(wd, wd0, local.at[6]).wait()
        for m in range(6):
            for kind in range(5):
                copy(m, kind).wait_send()


def first(x, bg, bu, bd, tm=512):
    t, d = x.shape
    f = bg.shape[2]
    row = lambda n: pl.BlockSpec((tm, n), lambda i: (i, 0))
    once = lambda b: pl.BlockSpec(b.shape, lambda i: (0, 0, 0), pipeline_mode=pl.Buffered(1))
    hbm = pl.BlockSpec(memory_space=pl.ANY)
    out = jax.ShapeDtypeStruct
    return pl.pallas_call(
        first_kernel,
        grid=(t // tm,),
        in_specs=[row(d), once(bg), once(bu), once(bd)],
        out_specs=[row(d), row(f), row(f), row(f), row(d), hbm, hbm, hbm, hbm],
        out_shape=[
            out((t, d), bf16),
            out((t, f), bf16),
            out((t, f), f32),
            out((t, f), f32),
            out((t, d), bf16),
            out((d, f), bf16),
            out((d, f), bf16),
            out((f, d), bf16),
            out((f, d), bf16),
        ],
        scratch_shapes=[
            pltpu.VMEM((d, f), bf16),
            pltpu.VMEM((d, f), bf16),
            pltpu.VMEM((f, d), bf16),
            pltpu.VMEM((tm, f), bf16),
            pltpu.SemaphoreType.DMA((6, 5)),
            pltpu.SemaphoreType.DMA((6, 5)),
            pltpu.SemaphoreType.DMA((7,)),
        ],
        compiler_params=pltpu.CompilerParams(collective_id=1, has_side_effects=True, vmem_limit_bytes=62 * MIB),
        cost_estimate=pl.CostEstimate(flops=6 * t * d * f, bytes_accessed=120 * MIB, transcendentals=0),
        name="first_layer",
    )(x, bg, bu, bd)


def second_kernel(h_ref, dy_ref, g0, u0, wg, wu, wd, wd0, a_ref, act_ref, dgu_ref, dh_ref):
    f = wg.shape[1]
    h, dy = h_ref[...], dy_ref[...]
    wide, scale, a = normed(h)
    a_ref[...] = a
    by_gate = by_up = None
    for k in range(3):
        cols = slice(k * 768, (k + 1) * 768)
        gate, up = nn(a, wg[:, cols]), nn(a, wu[:, cols])
        dact = nt(dy, wd[cols, :]).astype(bf16).astype(f32)
        silu, dg, du = backward(dact, gate, up)
        spread(act_ref, k, (silu * up).astype(bf16))
        dg, du = dg.astype(bf16), du.astype(bf16)
        dgu_ref[:, k * 768 : (k + 1) * 768] = dg
        dgu_ref[:, f + k * 768 : f + (k + 1) * 768] = du
        part_gate, part_up = nt(dg, wg[:, cols]), nt(du, wu[:, cols])
        by_gate = part_gate if by_gate is None else by_gate + part_gate
        by_up = part_up if by_up is None else by_up + part_up
    da = (by_gate.astype(bf16) + by_up.astype(bf16)).astype(f32)
    along = jnp.mean(da * wide, -1, keepdims=True)
    dh = dy + (da * scale - wide * (scale * scale * scale * along)).astype(bf16)
    dh_ref[...] = dh
    for k in range(3):
        cols = slice(k * 768, (k + 1) * 768)
        dact = nt(dh, wd0[cols, :]).astype(bf16).astype(f32)
        _, dg, du = backward(dact, g0[:, cols], u0[:, cols])
        dgu_ref[:, 2 * f + k * 768 : 2 * f + (k + 1) * 768] = dg.astype(bf16)
        dgu_ref[:, 3 * f + k * 768 : 3 * f + (k + 1) * 768] = du.astype(bf16)


def second(h, dy, g0, u0, wg, wu, wd, wd0, tm=256):
    t, d = h.shape
    f = wg.shape[1]
    row = lambda n: pl.BlockSpec((tm, n), lambda i: (i, 0))
    once = lambda w: pl.BlockSpec(w.shape, lambda i: (0, 0), pipeline_mode=pl.Buffered(1))
    out = jax.ShapeDtypeStruct
    return pl.pallas_call(
        second_kernel,
        grid=(t // tm,),
        in_specs=[row(d), row(d), row(f), row(f), once(wg), once(wu), once(wd), once(wd0)],
        out_specs=[row(d), row(f), row(4 * f), row(d)],
        out_shape=[out((t, n), bf16) for n in (d, f, 4 * f, d)],
        compiler_params=pltpu.CompilerParams(vmem_limit_bytes=63 * MIB),
        cost_estimate=pl.CostEstimate(flops=12 * t * d * f, bytes_accessed=200 * MIB, transcendentals=0),
        name="second_layer",
    )(h, dy, g0, u0, wg, wu, wd, wd0)


UNITS, LAGS = 24, {"C": 2, "X": 4, "Y": 6, "Z": 8, "A": 10, "B": 12}


def sum_kernel(
    a1, dy, dh, a0, dgu, act1, act0, og, od, osq, res, tile, g, rc, kx, sx, rx, ky, sy, ry, fg, fd, sg, sd, rzg, rzd, outg, outd, square,
    csem, xsem, ysem, zsem, asem, bsem, rsem, tsem, osem,
):
    t = pl.program_id(0)
    r, s = lax.axis_index("r"), lax.axis_index("s")
    x, c, y, z = s // 2, s % 2, r // 4, r % 4
    core, across, other = s + 1 - 2 * c, lax.rem(s + 2, 4), lax.rem(r + 4, 8)
    peers = [y * 4 + lax.rem(z + k, 4) for k in (1, 2, 3)]
    down = lambda u: (u >= 9) & (u < 15)
    of_gate = lambda u: jnp.where(u < 9, u, u - 6)

    def remote(src, dst, sem, rr, ss):
        return pltpu.make_async_remote_copy(
            src_ref=src, dst_ref=dst, send_sem=sem[0], recv_sem=sem[1], device_id=(0, rr, ss), device_id_type=MESH
        )

    def pick(sem, *at):
        return sem.at[(0, *at)], sem.at[(1, *at)]

    class Kind:
        def __init__(self, u, is_down):
            self.u, self.down = u, is_down
            self.rows, self.cols = (96, 896) if is_down else (112, 512)
            self.two, self.four = lax.rem(u, 2), lax.rem(u, 4)
            self.box = (slice(None, self.rows), slice(None, self.cols))
            self.cut = (pl.ds(0, self.rows), pl.ds(0, self.cols))
            self.index = u - 9 if is_down else of_gate(u)
            self.full, self.send, self.got, self.out = (fd, sd, rzd, outd) if is_down else (fg, sg, rzg, outg)

        def c_copy(self):
            b = self.two
            everything = (slice(None), slice(None), *self.cut)
            return remote(g.at[(b, 1 - c, *everything)], rc.at[(b, *everything)], pick(csem, self.four), r, core)

        def x_copy(self):
            everything = (slice(None), *self.cut)
            return remote(
                sx.at[(self.two, *everything)], rx.at[(self.four, *everything)], pick(xsem, self.four), r, across
            )

        def y_copy(self):
            return remote(sy.at[(self.two, *self.cut)], ry.at[(self.four, *self.cut)], pick(ysem, self.four), other, s)

        def z_copies(self):
            return [
                remote(
                    self.send.at[self.two, lax.rem(z + k + 1, 4)],
                    self.got.at[self.four, k],
                    pick(zsem, self.four, k),
                    peers[k],
                    s,
                )
                for k in range(3)
            ]

        def a_copies(self):
            mine = self.out.at[self.index, y, z]
            return [remote(mine, mine, pick(asem, self.four, k), peers[k], s) for k in range(3)]

        def b_copy(self):
            mine = self.out.at[self.index, y]
            return remote(mine, mine, pick(bsem, self.four), other, s)

        def put_out(self):
            return pltpu.make_async_copy(
                self.out.at[self.index], (od if self.down else og).at[self.index], osem.at[self.u]
            )

    def both(u, work):
        here = (u >= 0) & (u < UNITS)

        @pl.when(here & jnp.logical_not(down(u)))
        def _():
            work(Kind(u, False))

        @pl.when(here & down(u))
        def _():
            work(Kind(u, True))

    def tile_copy(u, start):
        slot = lax.rem(u, 2)

        def act(copy):
            copy.start() if start else copy.wait()

        @pl.when((u < UNITS) & jnp.logical_not(down(u)))
        def _():
            first = pl.multiple_of(of_gate(u) * 512, 512)
            act(pltpu.make_async_copy(dgu.at[:, pl.ds(first, 512)], tile.at[slot, :, pl.ds(0, 512)], tsem.at[slot]))

        for source, base in ((act1, 9), (act0, 12)):

            @pl.when((u >= base) & (u < base + 3))
            def _():
                first = pl.multiple_of((u - base) * 768, 768)
                act(pltpu.make_async_copy(source.at[:, pl.ds(first, 768)], tile.at[slot], tsem.at[slot]))

    held = [pltpu.make_async_copy(src, res.at[k % 2], rsem.at[k]) for k, src in enumerate((a1, dy, dh, a0))]

    @pl.when(t == 0)
    def _():
        held[0].start()
        tile_copy(t, True)
        held[1].start()
        square[...] = jnp.zeros_like(square)
        barrier = pltpu.get_barrier_semaphore()
        for rr, ss in ((r, core), (r, across), (other, s), (peers[0], s), (peers[1], s), (peers[2], s)):
            pl.semaphore_signal(barrier, inc=1, device_id=(0, rr, ss), device_id_type=MESH)
        pl.semaphore_wait(barrier, 6)
        held[0].wait()

    def b_wait(k):
        k.b_copy().wait()
        k.put_out().start()

    def a_wait(k):
        for copy in k.a_copies():
            copy.wait()
        k.b_copy().start()

    def z_wait(k):
        for copy in k.z_copies():
            copy.wait()
        total = k.full[k.two, z]
        for i in range(3):
            total += k.got[k.four, i].astype(f32)
        rounded = total.astype(bf16)
        k.out[k.index, y, z] = rounded
        wide = rounded.astype(f32)
        wide = wide * wide
        total = square[...]
        for i in range(wide.shape[0] // 8):
            for j in range(wide.shape[1] // 128):
                total += wide[8 * i : 8 * i + 8, 128 * j : 128 * j + 128]
        square[...] = total
        for copy in k.a_copies():
            copy.start()

    def y_wait(k):
        k.y_copy().wait()
        for i in range(4):
            if k.down:
                at = (slice(24 * i, 24 * i + 24), slice(None, 896))
            else:
                at = (slice(None, 112), slice(128 * i, 128 * i + 128))
            total = ky[(k.two, *at)] + ry[(k.four, *at)].astype(f32)
            k.full[k.two, i] = total
            k.send[k.two, i] = total.astype(bf16)
        for copy in k.z_copies():
            copy.start()

    def x_wait(k):
        k.x_copy().wait()
        ky[(k.two, *k.box)] = kx[(k.two, y, *k.box)] + rx[(k.four, y, *k.box)].astype(f32)
        away = kx[(k.two, 1 - y, *k.box)] + rx[(k.four, 1 - y, *k.box)].astype(f32)
        sy[(k.two, *k.box)] = away.astype(bf16)
        k.y_copy().start()

    def c_wait(k):
        k.c_copy().wait()
        for i in range(2):
            away = g[(k.two, c, 1 - x, i, *k.box)].astype(f32) + rc[(k.two, 1 - x, i, *k.box)].astype(f32)
            sx[(k.two, i, *k.box)] = away.astype(bf16)
        k.x_copy().start()
        for i in range(2):
            kx[(k.two, i, *k.box)] = g[(k.two, c, x, i, *k.box)].astype(f32) + rc[(k.two, x, i, *k.box)].astype(f32)

    both(t - LAGS["B"], b_wait)
    both(t - LAGS["A"], a_wait)
    both(t - LAGS["Z"], z_wait)
    both(t - LAGS["Y"], y_wait)
    both(t - LAGS["X"], x_wait)
    both(t - LAGS["C"], c_wait)
    both(t - 1, lambda k: k.c_copy().start())

    for k, when in ((1, 9), (2, 12), (3, 15)):

        @pl.when(t == when)
        def _():
            held[k].wait()
            if k < 3:
                held[k + 1].start()

    def store(k, product):
        for block in range(4):
            for half in range(2):
                first = (2 * block + half) * k.rows
                g[(k.two, block % 2, block // 2, half, *k.box)] = product[first : first + k.rows].astype(bf16)

    @pl.when(t < UNITS)
    def _():
        tile_copy(t, False)
        tile_copy(t + 1, True)
        slot = lax.rem(t, 2)

        @pl.when(jnp.logical_not(down(t)))
        def _():
            store(Kind(t, False), tn(res[jnp.where(t < 9, 0, 1)], tile[slot, :, :512]))

        @pl.when(down(t))
        def _():
            store(Kind(t, True), tn(tile[slot], res[jnp.where(t < 12, 1, 0)]))

    @pl.when(t == pl.num_programs(0) - 1)
    def _():
        osq[...] = square[...]
        for u in range(UNITS):
            Kind(u, 9 <= u < 15).put_out().wait()


def summed(a1, dy, dh, a0, dgu, act1, act0):
    t, d = a1.shape
    hbm = pl.BlockSpec(memory_space=pl.ANY)
    out, vmem, dma = jax.ShapeDtypeStruct, pltpu.VMEM, pltpu.SemaphoreType.DMA
    og, od = (18, 2, 4, 112, 128), (6, 2, 4, 24, 896)
    part = (112, 896)
    return pl.pallas_call(
        sum_kernel,
        grid=(UNITS + LAGS["B"],),
        in_specs=[hbm] * 7,
        out_specs=[hbm, hbm, pl.BlockSpec((8, 128), lambda i: (0, 0))],
        out_shape=[out(og, bf16), out(od, bf16), out((8, 128), f32)],
        scratch_shapes=[
            vmem((2, t, d), bf16),
            vmem((2, t, 768), bf16),
            vmem((2, 2, 2, 2, *part), bf16),
            vmem((2, 2, 2, *part), bf16),
            vmem((2, 2, *part), f32),
            vmem((2, 2, *part), bf16),
            vmem((4, 2, *part), bf16),
            vmem((2, *part), f32),
            vmem((2, *part), bf16),
            vmem((4, *part), bf16),
            vmem((2, *og[2:]), f32),
            vmem((2, *od[2:]), f32),
            vmem((2, *og[2:]), bf16),
            vmem((2, *od[2:]), bf16),
            vmem((4, 3, *og[3:]), bf16),
            vmem((4, 3, *od[3:]), bf16),
            vmem(og, bf16),
            vmem(od, bf16),
            vmem((8, 128), f32),
            dma((2, 4)),
            dma((2, 4)),
            dma((2, 4)),
            dma((2, 4, 3)),
            dma((2, 4, 3)),
            dma((2, 4)),
            dma((4,)),
            dma((2,)),
            dma((UNITS,)),
        ],
        compiler_params=pltpu.CompilerParams(collective_id=2, has_side_effects=True, vmem_limit_bytes=63 * MIB),
        name="sums",
    )(a1, dy, dh, a0, dgu, act1, act0)


def adamw(w, m, v, g):
    m = 0.9 * m + 0.1 * g
    v = 0.95 * v + 0.05 * g * g
    step = m * lax.rsqrt(v + 1e-8) + 0.1 * w
    return (w - 0.02 * step).astype(bf16), m, v


def solution(mesh):
    def step(x, dy, wg, wu, wd, *state):
        x, dy = x[0], dy[0]
        a0, act0, g0, u0, h, wg1, wu1, wd1, wd0 = first(x, wg, wu, wd)
        a1, act1, dgu, dh = second(h, dy, g0, u0, wg1, wu1, wd1, wd0)
        og, od, squares = summed(a1, dy, dh, a0, dgu, act1, act0)
        squares = lax.psum(jnp.sum(squares), ("r", "s"))
        gu = og.reshape(2, 9, 2, 4, 112, 128).transpose(0, 2, 4, 1, 3, 5).reshape(2, *wg.shape[1:2], 2, wg.shape[2])
        gate, up = gu[::-1, :, 0], gu[::-1, :, 1]
        dn = od.reshape(wd.shape)[::-1]
        gradients = [g.astype(f32) for g in (gate, up, dn)]
        count = 4 * sum(g.size for g in gradients)
        factor = jnp.minimum(1.0, 0.5 * lax.rsqrt(squares / count + 1e-30))
        new = [
            adamw(w.astype(f32), m, v, g * factor)
            for w, m, v, g in zip((wg, wu, wd), state[:3], state[3:], gradients, strict=True)
        ]
        return tuple(one[which] for which in range(3) for one in new)

    states, cut = P(("rep", "r", "s"), None, None), P(None, "s", None)
    return jax.shard_map(
        step,
        mesh=mesh,
        in_specs=(states, states) + (cut,) * 9,
        out_specs=(P("rep", "s", None),) * 9,
        check_vma=False,
    )
```
